128 devices in a mesh: expert: 4 (over y_lo, core), shard: 32 (over z, y_hi, x).
Axes of the slice: x: 4, y: 4 (y_hi: 2, y_lo: 2; y = y_hi * 2 + y_lo), z: 4, core: 2. Of those that a mesh axis runs over, the one named last changes fastest.
Arguments:
- train_down: float32 [16, 6400, 4096], P('expert', None, 'shard'), may hold values from -0.15625 to 0.15625
- other_down: bfloat16 [16, 6400, 4096], P('expert', None, 'shard'), may hold values from -0.0390625 to 0.0390625
- router_weight: float32 [4096, 16], P('shard', 'expert'), may hold values from -0.09375 to 0.09375
- router_gain: float32 [4096], P('shard'), may hold values from 0.25 to 1.75
Outputs:
- ready_down: bfloat16 [16, 6400, 4096], P('expert', 'shard')
- scale_down: float32 [16, 6400], P('expert', 'shard')
- serve_router: bfloat16 [4096, 16], replicated
The draws below stay inside these ranges and needn't reach their ends.
All inputs are finite; a program needn't handle non-finite values.
Results may differ from the reference program's by a relative error of at most 0.001.
Values may be sent and summed in bfloat16 or wider, within the bound.
A program may use at most 128 MiB of HBM per device.

```python
import jax
import jax.numpy as jnp
from jax import lax

EXPERTS = 16
D_MODEL = 4096
D_EXPERT = 6400


def with_spikes(array, rng, source, target, parts, factor):
    def block_of(axis_at):
        return (jnp.arange(array.shape[axis_at]) // (array.shape[axis_at] // parts)).reshape((-1,) + (1,) * (array.ndim - 1 - axis_at))

    first = jax.random.permutation(rng, parts)[block_of(target)]
    far = (block_of(target) + parts // 2) % parts
    return jnp.where((block_of(source) == first) | (block_of(source) == far), factor * array, array)


def block_levels(own_key, shape, cuts, low, high):
    gain = 1.0
    for axis_at, shards_of in cuts:
        steps = jax.random.uniform(jax.random.fold_in(jax.random.fold_in(own_key, 6), axis_at), (shards_of,), jnp.float32, low / len(cuts), high / len(cuts))
        gain = gain * jnp.repeat(jnp.exp(steps), shape[axis_at] // shards_of).reshape((-1,) + (1,) * (len(shape) - 1 - axis_at))
    return gain


def centred(rng, extent, deviation, bound, shards=(), held_as=jnp.bfloat16):
    result = jax.random.normal(rng, extent, jnp.float32) * deviation
    if len(shards) > 0:
        result = block_levels(rng, extent, shards, -0.22, 0.18) * result
    return jnp.clip(result, min=-bound, max=bound).astype(held_as)


def bell_draw_with(key, dims, deviation, reach, pieces, heavy, held_as=jnp.bfloat16):
    entries = deviation * jax.random.normal(key, dims, jnp.float32)
    if pieces:
        entries = entries * block_levels(key, dims, pieces, -0.22, 0.18)
    return jnp.clip(with_spikes(entries, jax.random.fold_in(key, 3), *heavy), -reach, reach).astype(held_as)


def setup_inputs(seed: int = 0) -> dict:
    key_of = jax.random.split(jax.random.key(seed), 5)
    return {
        "train_down": bell_draw_with(key_of[0], (EXPERTS, D_EXPERT, D_MODEL), D_EXPERT ** -0.5, 0.15625, ((0, 4), (2, 32)), (2, 1, 32, 2.75), jnp.float32),
        "other_down": centred(key_of[1], (EXPERTS, D_EXPERT, D_MODEL), (D_EXPERT * 4) ** -0.5, 0.0390625, ((0, 4), (2, 32))),
        "router_weight": centred(key_of[2], (D_MODEL, EXPERTS), D_MODEL ** -0.5, 0.09375, ((0, 32), (1, 4)), jnp.float32),
        "router_gain": jnp.clip(1.0 + 0.15 * jax.random.normal(key_of[3], (D_MODEL,), jnp.float32), 0.25, 1.75),
    }


def reference(train_down, other_down, router_weight, router_gain):
    latest_down = train_down + other_down.astype(jnp.float32)
    scale_down = jnp.sqrt(lax.optimization_barrier(jnp.sum(latest_down * latest_down, axis=2)))
    ready_down = (latest_down / jnp.expand_dims(scale_down, 2)).astype(jnp.bfloat16)
    serve_router = (router_weight * router_gain[:, None]).astype(jnp.bfloat16)
    return (ready_down, scale_down, serve_router)
```

```python
import functools

import jax
import jax.numpy as jnp
from jax import lax
from jax.experimental import pallas as pl
from jax.experimental.pallas import tpu as pltpu
from jax.sharding import PartitionSpec as P

MESH = pl.DeviceIdType.MESH
F32 = jnp.float32
BF16 = jnp.bfloat16
SPAN = 240.0
HALF = 120.0
LN2 = 0.6931471805599453
TINY = 1e-37


def coords(shard):
    return shard // 8, (shard // 4) % 2, shard % 4


def ahead(me, off):
    z, y, x = coords(me)
    dz, dy, dx = coords(off)
    return ((z + dz) % 4) * 8 + ((y + dy) % 2) * 4 + (x + dx) % 4


def behind(me, off):
    z, y, x = coords(me)
    dz, dy, dx = coords(off)
    return ((z + 4 - dz) % 4) * 8 + ((y + 2 - dy) % 2) * 4 + (x + 4 - dx) % 4


def turn(i, e):
    return (27 * i + 9 * e) % 32


def to_all_lanes(tile, lane):
    return jnp.broadcast_to(tile[:, lane : lane + 1], tile.shape)


def exchange(train, other, weight, gain, ready, scale, router,
             tbuf, obuf, sbuf, rbuf, ssum, rsum, fbuf, part, pair, rows_in, rows_out,
             load_t, load_o, send, recv, self_sem, sum_send, sum_recv,
             pair_send, pair_recv, row_send, row_recv, core_send, core_recv):
    experts, tiles = ready.shape[0], ready.shape[1]
    me = lax.axis_index("shard")
    group = lax.axis_index("expert")
    y_lo, core = group // 2, group % 2
    across = (1 - y_lo) * 2 + core
    beside = y_lo * 2 + (1 - core)

    loads = []
    for e in range(experts):
        pair_of = (
            pltpu.make_async_copy(train.at[e], tbuf.at[e], load_t.at[e]),
            pltpu.make_async_copy(other.at[e], obuf.at[e], load_o.at[e]),
        )
        for copy in pair_of:
            copy.start()
        loads.append(pair_of)

    barrier = pltpu.get_barrier_semaphore()

    def greet(off, _):
        pl.semaphore_signal(barrier, inc=1, device_id={"shard": ahead(me, off)}, device_id_type=MESH)
        return 0

    lax.fori_loop(1, 32, greet, 0)
    for peer in (across, beside):
        pl.semaphore_signal(barrier, inc=1, device_id={"expert": peer}, device_id_type=MESH)

    lanes = lax.broadcasted_iota(jnp.int32, (8, 128), 1)

    def latest(e, j, t):
        at = j * tiles + t
        return tbuf[e, at] + obuf[e, at].astype(F32)

    def sums_of(e):
        def body(off, _):
            j = ahead(me, off)
            tile = jnp.zeros((8, 128), F32) if e == 0 else ssum[off]
            for t in range(tiles):
                x = latest(e, j, t)
                total = jnp.sum(x * x, axis=1, keepdims=True)
                tile = jnp.where(lanes == e * tiles + t, total, tile)
            ssum[off] = tile
            return 0

        for copy in loads[e]:
            copy.wait()
        lax.fori_loop(0, 32, body, 0)

    def send_piece(e, off):
        p = e * 32 + off

        @pl.when(off != 0)
        def _():
            pltpu.make_async_remote_copy(
                sbuf.at[p], rbuf.at[p], send, recv.at[p],
                device_id={"shard": ahead(me, off)}, device_id_type=MESH,
            ).start()

    def encode(e):
        def body(i, _):
            off = turn(i, e)
            p = e * 32 + off
            j = ahead(me, off)
            inverse = lax.rsqrt(jnp.maximum(ssum[off], TINY))
            for t in range(tiles):
                x = latest(e, j, t)
                share = jnp.maximum(jnp.abs(x) * to_all_lanes(inverse, e * tiles + t), 1e-30)
                root = share * lax.rsqrt(share)
                code = jnp.exp2(root * SPAN - HALF)
                sbuf[p, t] = jnp.where(x < 0, -code, code).astype(BF16)

            @pl.when(i > 0)
            def _():
                send_piece(e, turn(i + 31, e))

            return 0

        lax.fori_loop(0, 32, body, 0)
        send_piece(e, turn(31, e))

    own = weight[...] * gain[...]
    part[...] = jnp.concatenate([own, jnp.zeros_like(own)], axis=0).astype(BF16)

    sums_of(0)
    pl.semaphore_wait(barrier, 33)
    to_pair = pltpu.make_async_remote_copy(
        part, pair, pair_send, pair_recv, device_id={"expert": across}, device_id_type=MESH
    )
    to_pair.start()
    encode(0)
    for e in range(1, experts):
        sums_of(e)

    to_pair.wait()
    mine, theirs = part[...].astype(F32)[:4], pair[...].astype(F32)[:4]
    low = jnp.where(y_lo == 0, mine, theirs)
    high = jnp.where(y_lo == 0, theirs, mine)
    rows_in[0] = jnp.concatenate([low, high], axis=0).astype(BF16)
    rsum[0] = ssum[0]

    def send_small(i, _):
        off = turn(i, 0)

        @pl.when(off != 0)
        def _():
            pltpu.make_async_remote_copy(
                ssum.at[off], rsum.at[off], sum_send, sum_recv,
                device_id={"shard": ahead(me, off)}, device_id_type=MESH,
            ).start()
            pltpu.make_async_remote_copy(
                rows_in.at[0], rows_in.at[off], row_send, row_recv,
                device_id={"shard": ahead(me, off)}, device_id_type=MESH,
            ).start()

        return 0

    lax.fori_loop(0, 32, send_small, 0)
    for e in range(1, experts):
        encode(e)
    keep = [
        pltpu.make_async_copy(sbuf.at[e * 32], rbuf.at[e * 32], self_sem.at[e])
        for e in range(experts)
    ]
    for copy in keep:
        copy.start()

    rest = pltpu.make_async_remote_copy(
        ssum.at[pl.ds(1, 31)], rsum.at[pl.ds(1, 31)], sum_send, sum_recv,
        device_id={"shard": ahead(me, 1)}, device_id_type=MESH,
    )
    rest.wait_recv()
    total = lax.fori_loop(1, 32, lambda k, acc: acc + rsum[k], rsum[0])

    def factors(k, _):
        fbuf[k] = jnp.sqrt(rsum[k] / total)
        return 0

    lax.fori_loop(0, 32, factors, 0)
    norm = jnp.sqrt(total)
    wide = lax.broadcasted_iota(jnp.int32, (8, 256), 1) - lax.broadcasted_iota(jnp.int32, (8, 256), 0)
    for e in range(experts):
        spread = jnp.zeros((8, 256), F32)
        for t in range(tiles):
            column = norm[:, e * tiles + t : e * tiles + t + 1]
            spread = jnp.where(wide == t * 8, column, spread)
        scale[e : e + 1, :] = jnp.sum(spread, axis=0, keepdims=True)[:, : tiles * 8]

    def decode(e):
        def body(i, _):
            off = turn(i, e)
            p = e * 32 + off
            source = behind(me, off)

            @pl.when(off != 0)
            def _():
                pltpu.make_async_remote_copy(
                    sbuf.at[p], rbuf.at[p], send, recv.at[p],
                    device_id={"shard": source}, device_id_type=MESH,
                ).wait_recv()

            factor = fbuf[off]
            for t in range(tiles):
                y = rbuf[p, t].astype(F32)
                root = jnp.log(jnp.abs(y)) * (1.0 / (SPAN * LN2)) + HALF / SPAN
                value = root * root * to_all_lanes(factor, e * tiles + t)
                ready[e, t, source] = jnp.where(y < 0, -value, value).astype(BF16)
            return 0

        keep[e].wait()
        lax.fori_loop(0, 32, body, 0)

    decode(0)
    rows = pltpu.make_async_remote_copy(
        rows_in.at[pl.ds(1, 31)], rows_in.at[pl.ds(1, 31)], row_send, row_recv,
        device_id={"shard": ahead(me, 1)}, device_id_type=MESH,
    )
    rows.wait_recv()
    to_core = pltpu.make_async_remote_copy(
        rows_in, rows_out, core_send, core_recv, device_id={"expert": beside}, device_id_type=MESH
    )
    to_core.start()
    decode(1)
    to_core.wait()

    def place(k, _):
        a, b = rows_in[k].astype(F32), rows_out[k].astype(F32)
        first = jnp.where(core == 0, a, b)
        second = jnp.where(core == 0, b, a)
        block = jnp.concatenate([first[:4], second[:4], first[4:], second[4:]], axis=0)
        router[:, pl.ds(pl.multiple_of(behind(me, k) * 128, 128), 128)] = block.astype(BF16)
        return 0

    lax.fori_loop(0, 32, place, 0)
    for e in range(2, experts):
        decode(e)

    rest.wait_send()
    pltpu.make_async_remote_copy(
        rows_in.at[pl.ds(1, 31)], rows_in.at[pl.ds(1, 31)], row_send, row_recv,
        device_id={"shard": ahead(me, 1)}, device_id_type=MESH,
    ).wait_send()
    pltpu.make_async_remote_copy(
        sbuf.at[pl.ds(0, 31 * experts)], rbuf.at[pl.ds(0, 31 * experts)], send, recv.at[0],
        device_id={"shard": ahead(me, 1)}, device_id_type=MESH,
    ).wait_send()


def deliver(ready_in, scale_in, router_in, ready, scale, router, sems):
    copies = [
        pltpu.make_async_copy(ready_in.at[e], ready.at[e], sems.at[e]) for e in range(ready.shape[0])
    ]
    for copy in copies:
        copy.start()
    scale[...] = scale_in[...]
    router[...] = router_in[...]
    for copy in copies:
        copy.wait()


def per_device(train_down, other_down, router_weight, router_gain):
    experts, inner, columns = train_down.shape
    tiles = inner // 32 // 8
    rows = inner // 8
    train = train_down.reshape(experts, rows, 8, columns)
    other = other_down.reshape(experts, rows, 8, columns)
    vmem = pl.BlockSpec(memory_space=pltpu.VMEM)
    anywhere = pl.BlockSpec(memory_space=pl.ANY)
    dma = pltpu.SemaphoreType.DMA
    pieces = experts * 32
    inside = pl.pallas_call(
        exchange,
        out_shape=(
            pltpu.VMEM((experts, tiles, 32, 8, columns), BF16),
            pltpu.VMEM((experts, tiles * 8), F32),
            pltpu.VMEM((16, 4096), BF16),
        ),
        in_specs=[anywhere, anywhere, vmem, vmem],
        out_specs=(vmem, vmem, vmem),
        scratch_shapes=[
            pltpu.VMEM((experts, rows, 8, columns), F32),
            pltpu.VMEM((experts, rows, 8, columns), BF16),
            pltpu.VMEM((pieces, tiles, 8, columns), BF16),
            pltpu.VMEM((pieces, tiles, 8, columns), BF16),
            pltpu.VMEM((32, 8, 128), F32),
            pltpu.VMEM((32, 8, 128), F32),
            pltpu.VMEM((32, 8, 128), F32),
            pltpu.VMEM((8, 128), BF16),
            pltpu.VMEM((8, 128), BF16),
            pltpu.VMEM((32, 8, 128), BF16),
            pltpu.VMEM((32, 8, 128), BF16),
            dma((experts,)), dma((experts,)), dma, dma((pieces,)), dma((experts,)),
            dma, dma, dma, dma, dma, dma, dma, dma,
        ],
        compiler_params=pltpu.CompilerParams(
            collective_id=0, has_side_effects=True, vmem_limit_bytes=48 * 1024 * 1024
        ),
        name="exchange",
    )(train, other, router_weight.T, router_gain.reshape(1, -1))
    ready, scale, router = pl.pallas_call(
        deliver,
        out_shape=(
            jax.ShapeDtypeStruct((experts, tiles, 32, 8, columns), BF16),
            jax.ShapeDtypeStruct((experts, tiles * 8), F32),
            jax.ShapeDtypeStruct((16, 4096), BF16),
        ),
        in_specs=[vmem, vmem, vmem],
        out_specs=(anywhere, vmem, vmem),
        scratch_shapes=[dma((experts,))],
        compiler_params=pltpu.CompilerParams(vmem_limit_bytes=16 * 1024 * 1024),
        name="deliver",
    )(*inside)
    ready = ready.transpose(0, 1, 3, 2, 4).reshape(experts, tiles * 8, 32 * columns)
    return (ready, scale, router.T)


def solution(mesh):
    in_specs = (
        P("expert", None, "shard"),
        P("expert", None, "shard"),
        P("shard", "expert"),
        P("shard"),
    )
    out_specs = (P("expert", "shard", None), P("expert", "shard"), P())
    return jax.shard_map(
        per_device, mesh=mesh, in_specs=in_specs, out_specs=out_specs, check_vma=False
    )
```

```python
import functools

import jax
import jax.numpy as jnp
from jax import lax
from jax.experimental import pallas as pl
from jax.experimental.pallas import tpu as pltpu
from jax.sharding import PartitionSpec as P

MESH = pl.DeviceIdType.MESH
F32 = jnp.float32
BF16 = jnp.bfloat16
SPAN = 240.0
HALF = 120.0
LN2 = 0.6931471805599453
TINY = 1e-37
CHUNKS = 5
WITH_SUMS = 1
EXTRA = 3


def coords(shard):
    return shard // 8, (shard // 4) % 2, shard % 4


def ahead(me, off):
    z, y, x = coords(me)
    dz, dy, dx = coords(off)
    return ((z + dz) % 4) * 8 + ((y + dy) % 2) * 4 + (x + dx) % 4


def behind(me, off):
    z, y, x = coords(me)
    dz, dy, dx = coords(off)
    return ((z + 4 - dz) % 4) * 8 + ((y + 2 - dy) % 2) * 4 + (x + 4 - dx) % 4


def steps_to(off):
    dz, dy, dx = coords(off)
    return min(dz, 4 - dz) + dy + min(dx, 4 - dx)


def in_words(k):
    offs = sorted(off for off in range(32) if steps_to(off) == k)
    offs = sorted(offs, key=lambda off: off * 11 % 32)
    return [offs[i : i + 5] for i in range(0, len(offs), 5)]


STAGES = [in_words(k) for k in range(1, 6)]
STAGES[-1][-1].append(0)
NEAR = STAGES[0][0]


def each(word, body):
    def step(_, rest):
        body(rest % 32)
        return rest // 32

    lax.fori_loop(0, len(word), step, jnp.int32(sum(off * 32**i for i, off in enumerate(word))))


def turn(i, e):
    return (27 * (i + 1) + 9 * e) % 32


def to_all_lanes(tile, lane):
    return jnp.broadcast_to(tile[:, lane : lane + 1], tile.shape)


def exchange(train, other, weight, gain, ready, scale, router,
             tbuf, obuf, sbuf, rbuf, ssum, fbuf, part, pair, own_rows, rows_in, rows_out,
             first_t, first_o, load_t, load_o, stage_sem, send, send_more, recv, self_sem,
             pair_send, pair_recv, core_send, core_recv):
    experts, tiles = ready.shape[0], ready.shape[1]
    me = lax.axis_index("shard")
    group = lax.axis_index("expert")
    y_lo, core = group // 2, group % 2
    across = (1 - y_lo) * 2 + core
    beside = y_lo * 2 + (1 - core)

    barrier = pltpu.get_barrier_semaphore()
    for off in NEAR:
        pl.semaphore_signal(barrier, inc=1, device_id={"shard": ahead(me, off)}, device_id_type=MESH)
    for peer in (across, beside):
        pl.semaphore_signal(barrier, inc=1, device_id={"expert": peer}, device_id_type=MESH)

    words = [word for stage in STAGES for word in stage]
    for w, word in enumerate(words):
        def load_piece(off):
            at = pl.ds(ahead(me, off) * tiles, tiles)
            pltpu.make_async_copy(train.at[0, at], tbuf.at[0, at], first_t.at[w]).start()
            pltpu.make_async_copy(other.at[0, at], obuf.at[0, at], first_o.at[w]).start()

        each(word, load_piece)

    def wait_first(w):
        at = pl.ds(0, len(words[w]) * tiles)
        pltpu.make_async_copy(train.at[0, at], tbuf.at[0, at], first_t.at[w]).wait()
        pltpu.make_async_copy(other.at[0, at], obuf.at[0, at], first_o.at[w]).wait()

    loads = []
    for e in range(1, experts):
        of_expert = []
        for c in range(CHUNKS):
            part_of = pl.ds(c * (tiles * 32 // CHUNKS), tiles * 32 // CHUNKS)
            k = (e - 1) * CHUNKS + c
            of_expert += [
                pltpu.make_async_copy(train.at[e, part_of], tbuf.at[e, part_of], load_t.at[k]),
                pltpu.make_async_copy(other.at[e, part_of], obuf.at[e, part_of], load_o.at[k]),
            ]
        loads.append(of_expert)

    lanes = lax.broadcasted_iota(jnp.int32, (8, 128), 1)

    def latest(e, j, t):
        at = j * tiles + t
        return tbuf[e, at] + obuf[e, at].astype(F32)

    def sums_of(e):
        def body(k, _):
            for off in [k * 4 + step for step in range(4)]:
                j = ahead(me, off)
                tile = ssum[off]
                for t in range(tiles):
                    x = latest(e, j, t)
                    total = jnp.sum(x * x, axis=1, keepdims=True)
                    tile = jnp.where(lanes == e * tiles + t, total, tile)
                ssum[off] = tile
            return 0

        for copy in loads[e - 1]:
            copy.wait()
        lax.fori_loop(0, 8, body, 0)

    def tiles_of(e):
        return pl.ds(0, tiles + EXTRA if e == WITH_SUMS else tiles)

    def piece(e, off, peer):
        at = (e * 32 + off, tiles_of(e))
        return pltpu.make_async_remote_copy(
            sbuf.at[at], rbuf.at[at], send_more if e == WITH_SUMS else send, recv.at[e * 32 + off],
            device_id={"shard": peer}, device_id_type=MESH,
        )

    def send_piece(e, off):
        @pl.when(off != 0)
        def _():
            piece(e, off, ahead(me, off)).start()

    def code(x, inverse):
        share = jnp.maximum(jnp.abs(x) * inverse, 1e-30)
        level = jnp.exp2(share * lax.rsqrt(share) * SPAN - HALF)
        return jnp.where(x < 0, -level, level).astype(BF16)

    def encode_first(off):
        j = ahead(me, off)
        tile = jnp.zeros((8, 128), F32)
        for t in range(tiles):
            x = latest(0, j, t)
            total = jnp.sum(x * x, axis=1, keepdims=True)
            tile = jnp.where(lanes == t, total, tile)
            sbuf[off, t] = code(x, lax.rsqrt(jnp.maximum(total, TINY)))
        ssum[off] = tile

    def encode(e, off):
        j = ahead(me, off)
        inverse = lax.rsqrt(jnp.maximum(ssum[off], TINY))
        for t in range(tiles):
            sbuf[e * 32 + off, t] = code(latest(e, j, t), to_all_lanes(inverse, e * tiles + t))
        if e == WITH_SUMS:
            high = ssum[off].astype(BF16)
            sbuf[e * 32 + off, tiles] = high
            sbuf[e * 32 + off, tiles + 1] = (ssum[off] - high.astype(F32)).astype(BF16)
            sbuf[e * 32 + off, tiles + 2] = own_rows[...]

    def encode_all(e):
        def body(k, _):
            for step in range(2):
                encode(e, turn(2 * k + step, e))

            @pl.when(k > 0)
            def _():
                for step in range(2):
                    send_piece(e, turn(2 * k - 2 + step, e))

            return 0

        lax.fori_loop(0, 16, body, 0)
        for i in (30, 31):
            send_piece(e, turn(i, e))

    own = weight[...] * gain[...]
    part[...] = jnp.concatenate([own, jnp.zeros_like(own)], axis=0).astype(BF16)

    to_pair = pltpu.make_async_remote_copy(
        part, pair, pair_send, pair_recv, device_id={"expert": across}, device_id_type=MESH
    )
    w = 0
    for k, stage in enumerate(STAGES):
        for first, word in zip([True] + [False] * len(stage), stage):
            wait_first(w)
            w += 1
            for off in word:
                encode_first(off)
            if first:
                if k == 0:
                    pl.semaphore_wait(barrier, len(NEAR) + 2)
                else:
                    pl.semaphore_wait(stage_sem.at[k - 1], len(NEAR))
                if k < len(STAGES) - 1:
                    for off in NEAR:
                        pl.semaphore_signal(
                            stage_sem.at[k], inc=1, device_id={"shard": ahead(me, off)}, device_id_type=MESH
                        )
            for off in word:
                if off:
                    send_piece(0, off)
        if k == 0:
            to_pair.start()
            for of_expert in loads:
                for copy in of_expert:
                    copy.start()

    for e in range(1, experts):
        sums_of(e)

    to_pair.wait()
    mine, theirs = part[...].astype(F32)[:4], pair[...].astype(F32)[:4]
    low = jnp.where(y_lo == 0, mine, theirs)
    high = jnp.where(y_lo == 0, theirs, mine)
    own_rows[...] = jnp.concatenate([low, high], axis=0).astype(BF16)

    for e in range(1, experts):
        encode_all(e)
    keep = []
    for e in range(experts):
        at = (e * 32, tiles_of(e))
        keep.append(pltpu.make_async_copy(sbuf.at[at], rbuf.at[at], self_sem.at[e]))
        keep[e].start()

    def arrival(e, off):
        @pl.when(off != 0)
        def _():
            piece(e, off, behind(me, off)).wait_recv()

    def arrive(i, _):
        arrival(WITH_SUMS, turn(i, WITH_SUMS))
        return 0

    def sums_from(k):
        p = WITH_SUMS * 32 + k
        return rbuf[p, tiles].astype(F32) + rbuf[p, tiles + 1].astype(F32)

    keep[WITH_SUMS].wait()
    lax.fori_loop(0, 32, arrive, 0)
    total = lax.fori_loop(1, 32, lambda k, acc: acc + sums_from(k), sums_from(0))

    def factors(k, _):
        fbuf[k] = jnp.sqrt(sums_from(k) / total)
        rows_in[k] = rbuf[WITH_SUMS * 32 + k, tiles + 2]
        return 0

    lax.fori_loop(0, 32, factors, 0)
    norm = jnp.sqrt(total)
    wide = lax.broadcasted_iota(jnp.int32, (8, 256), 1) - lax.broadcasted_iota(jnp.int32, (8, 256), 0)
    for e in range(experts):
        spread = jnp.zeros((8, 256), F32)
        for t in range(tiles):
            column = norm[:, e * tiles + t : e * tiles + t + 1]
            spread = jnp.where(wide == t * 8, column, spread)
        scale[e : e + 1, :] = jnp.sum(spread, axis=0, keepdims=True)[:, : tiles * 8]

    def decode(e):
        def body(k, _):
            offs = [turn(2 * k + step, e) for step in range(2)]
            if e != WITH_SUMS:
                for off in offs:
                    arrival(e, off)
            for off in offs:
                factor = fbuf[off]
                source = behind(me, off)
                for t in range(tiles):
                    y = rbuf[e * 32 + off, t].astype(F32)
                    root = jnp.log(jnp.abs(y)) * (1.0 / (SPAN * LN2)) + HALF / SPAN
                    value = root * root * to_all_lanes(factor, e * tiles + t)
                    ready[e, t, source] = jnp.where(y < 0, -value, value).astype(BF16)
            return 0

        if e != WITH_SUMS:
            keep[e].wait()
        lax.fori_loop(0, 16, body, 0)

    decode(1)
    to_core = pltpu.make_async_remote_copy(
        rows_in, rows_out, core_send, core_recv, device_id={"expert": beside}, device_id_type=MESH
    )
    to_core.start()
    decode(0)
    to_core.wait()

    def place(k, _):
        a, b = rows_in[k].astype(F32), rows_out[k].astype(F32)
        first = jnp.where(core == 0, a, b)
        second = jnp.where(core == 0, b, a)
        block = jnp.concatenate([first[:4], second[:4], first[4:], second[4:]], axis=0)
        router[:, pl.ds(pl.multiple_of(behind(me, k) * 128, 128), 128)] = block.astype(BF16)
        return 0

    lax.fori_loop(0, 32, place, 0)
    for e in range(2, experts):
        decode(e)

    others = [e for e in range(experts) if e != WITH_SUMS]
    at = (pl.ds(0, 31 * len(others)), pl.ds(0, tiles))
    pltpu.make_async_remote_copy(
        sbuf.at[at], rbuf.at[at], send, recv.at[0], device_id={"shard": ahead(me, 1)}, device_id_type=MESH
    ).wait_send()
    at = (pl.ds(0, 31), tiles_of(WITH_SUMS))
    pltpu.make_async_remote_copy(
        sbuf.at[at], rbuf.at[at], send_more, recv.at[0], device_id={"shard": ahead(me, 1)}, device_id_type=MESH
    ).wait_send()


def deliver(ready_in, scale_in, router_in, ready, scale, router, sems):
    experts, tiles = ready.shape[:2]
    copies = [
        pltpu.make_async_copy(scale_in, scale, sems.at[experts * CHUNKS]),
        pltpu.make_async_copy(router_in, router, sems.at[experts * CHUNKS + 1]),
    ]
    for k in range(experts * CHUNKS):
        at = (k // CHUNKS, pl.ds(k % CHUNKS * (tiles // CHUNKS), tiles // CHUNKS))
        copies.append(pltpu.make_async_copy(ready_in.at[at], ready.at[at], sems.at[k]))
    for copy in copies:
        copy.start()
    for copy in copies:
        copy.wait()


def per_device(train_down, other_down, router_weight, router_gain):
    experts, inner, columns = train_down.shape
    tiles = inner // 32 // 8
    rows = inner // 8
    train = train_down.reshape(experts, rows, 8, columns)
    other = other_down.reshape(experts, rows, 8, columns)
    vmem = pl.BlockSpec(memory_space=pltpu.VMEM)
    anywhere = pl.BlockSpec(memory_space=pl.ANY)
    dma = pltpu.SemaphoreType.DMA
    pieces = experts * 32
    inside = pl.pallas_call(
        exchange,
        out_shape=(
            pltpu.VMEM((experts, tiles, 32, 8, columns), BF16),
            pltpu.VMEM((experts, tiles * 8), F32),
            pltpu.VMEM((16, 4096), BF16),
        ),
        in_specs=[anywhere, anywhere, vmem, vmem],
        out_specs=(vmem, vmem, vmem),
        scratch_shapes=[
            pltpu.VMEM((experts, rows, 8, columns), F32),
            pltpu.VMEM((experts, rows, 8, columns), BF16),
            pltpu.VMEM((pieces, tiles + EXTRA, 8, columns), BF16),
            pltpu.VMEM((pieces, tiles + EXTRA, 8, columns), BF16),
            pltpu.VMEM((32, 8, 128), F32),
            pltpu.VMEM((32, 8, 128), F32),
            pltpu.VMEM((8, 128), BF16),
            pltpu.VMEM((8, 128), BF16),
            pltpu.VMEM((8, 128), BF16),
            pltpu.VMEM((32, 8, 128), BF16),
            pltpu.VMEM((32, 8, 128), BF16),
            dma((sum(map(len, STAGES)),)), dma((sum(map(len, STAGES)),)),
            dma(((experts - 1) * CHUNKS,)), dma(((experts - 1) * CHUNKS,)),
            pltpu.SemaphoreType.REGULAR((len(STAGES) - 1,)), dma, dma, dma((pieces,)), dma((experts,)),
            dma, dma, dma, dma,
        ],
        compiler_params=pltpu.CompilerParams(
            collective_id=0, has_side_effects=True, vmem_limit_bytes=48 * 1024 * 1024
        ),
        name="exchange",
    )(train, other, router_weight.T, router_gain.reshape(1, -1))
    ready, scale, router = pl.pallas_call(
        deliver,
        out_shape=(
            jax.ShapeDtypeStruct((experts, tiles, 32, 8, columns), BF16),
            jax.ShapeDtypeStruct((experts, tiles * 8), F32),
            jax.ShapeDtypeStruct((16, 4096), BF16),
        ),
        in_specs=[vmem, vmem, vmem],
        out_specs=(anywhere, anywhere, anywhere),
        scratch_shapes=[dma((experts * CHUNKS + 2,))],
        compiler_params=pltpu.CompilerParams(vmem_limit_bytes=16 * 1024 * 1024),
        name="deliver",
    )(*inside)
    ready = ready.transpose(0, 1, 3, 2, 4).reshape(experts, tiles * 8, 32 * columns)
    return (ready, scale, router.T)


def solution(mesh):
    in_specs = (
        P("expert", None, "shard"),
        P("expert", None, "shard"),
        P("shard", "expert"),
        P("shard"),
    )
    out_specs = (P("expert", "shard", None), P("expert", "shard"), P())
    return jax.shard_map(
        per_device, mesh=mesh, in_specs=in_specs, out_specs=out_specs, check_vma=False
    )
```

```python
import functools

import jax
import jax.numpy as jnp
from jax import lax
from jax.experimental import pallas as pl
from jax.experimental.pallas import tpu as pltpu
from jax.sharding import PartitionSpec as P

MESH = pl.DeviceIdType.MESH
F32 = jnp.float32
BF16 = jnp.bfloat16
SPAN = 240.0
HALF = 120.0
LN2 = 0.6931471805599453
TINY = 1e-37
CHUNKS = 5
ALONE = 2
WITH_ROWS = 2
EXTRA = 1
STRIDE = (27, 27, 27, 27)
SHIFT = (0, 14, 14, 29)


def coords(shard):
    return shard // 8, (shard // 4) % 2, shard % 4


def ahead(me, off):
    z, y, x = coords(me)
    dz, dy, dx = coords(off)
    return ((z + dz) % 4) * 8 + ((y + dy) % 2) * 4 + (x + dx) % 4


def behind(me, off):
    z, y, x = coords(me)
    dz, dy, dx = coords(off)
    return ((z + 4 - dz) % 4) * 8 + ((y + 2 - dy) % 2) * 4 + (x + 4 - dx) % 4


def steps_to(off):
    dz, dy, dx = coords(off)
    return min(dz, 4 - dz) + dy + min(dx, 4 - dx)


def in_words(k):
    offs = sorted(off for off in range(32) if steps_to(off) == k)
    offs = sorted(offs, key=lambda off: off * 11 % 32)
    return [offs[i : i + 5] for i in range(0, len(offs), 5)]


STAGES = [in_words(k) for k in range(1, 6)]
STAGES[-1][-1].append(0)
NEAR = STAGES[0][0]


def each(word, body):
    def step(_, rest):
        body(rest % 32)
        return rest // 32

    lax.fori_loop(0, len(word), step, jnp.int32(sum(off * 32**i for i, off in enumerate(word))))


def turn(i, e):
    return (STRIDE[e] * (i + 1) + SHIFT[e]) % 32


def to_all_lanes(tile, lane):
    return jnp.broadcast_to(tile[:, lane : lane + 1], tile.shape)


def exchange(train, other, weight_in, gain_in, ready, scale, router,
             weight, gain, small_sem, tbuf, obuf, sbuf, rbuf, ssum, rsum, fbuf, part, pair, own_rows, rows_in, rows_out,
             first_t, first_o, load_t, load_o, stage_sem, send, send_more, recv, self_sem,
             sum_send, sum_recv, pair_send, pair_recv, core_send, core_recv):
    experts, tiles = ready.shape[0], ready.shape[1]
    me = lax.axis_index("shard")
    group = lax.axis_index("expert")
    y_lo, core = group // 2, group % 2
    across = (1 - y_lo) * 2 + core
    beside = y_lo * 2 + (1 - core)

    barrier = pltpu.get_barrier_semaphore()
    for off in NEAR:
        pl.semaphore_signal(barrier, inc=1, device_id={"shard": ahead(me, off)}, device_id_type=MESH)
    for peer in (across, beside):
        pl.semaphore_signal(barrier, inc=1, device_id={"expert": peer}, device_id_type=MESH)

    words = [word for stage in STAGES for word in stage]
    for w, word in enumerate(words):
        def load_piece(off):
            at = pl.ds(ahead(me, off) * tiles, tiles)
            pltpu.make_async_copy(train.at[0, at], tbuf.at[0, at], first_t.at[w]).start()
            pltpu.make_async_copy(other.at[0, at], obuf.at[0, at], first_o.at[w]).start()

        each(word, load_piece)

    def wait_first(w):
        at = pl.ds(0, len(words[w]) * tiles)
        pltpu.make_async_copy(train.at[0, at], tbuf.at[0, at], first_t.at[w]).wait()
        pltpu.make_async_copy(other.at[0, at], obuf.at[0, at], first_o.at[w]).wait()

    loads = []
    for e in range(1, experts):
        of_expert = []
        for c in range(CHUNKS):
            part_of = pl.ds(c * (tiles * 32 // CHUNKS), tiles * 32 // CHUNKS)
            k = (e - 1) * CHUNKS + c
            of_expert += [
                pltpu.make_async_copy(train.at[e, part_of], tbuf.at[e, part_of], load_t.at[k]),
                pltpu.make_async_copy(other.at[e, part_of], obuf.at[e, part_of], load_o.at[k]),
            ]
        loads.append(of_expert)

    lanes = lax.broadcasted_iota(jnp.int32, (8, 128), 1)

    def latest(e, j, t):
        at = j * tiles + t
        return tbuf[e, at] + obuf[e, at].astype(F32)

    def sums_of(e):
        def body(k, _):
            for off in [k * 4 + step for step in range(4)]:
                j = ahead(me, off)
                tile = ssum[off]
                for t in range(tiles):
                    x = latest(e, j, t)
                    total = jnp.sum(x * x, axis=1, keepdims=True)
                    tile = jnp.where(lanes == e * tiles + t, total, tile)
                ssum[off] = tile
            return 0

        for copy in loads[e - 1]:
            copy.wait()
        lax.fori_loop(0, 8, body, 0)

    def tiles_of(e):
        return pl.ds(0, tiles + EXTRA if e == WITH_ROWS else tiles)

    def piece(e, off, peer):
        at = (e * 32 + off, tiles_of(e))
        return pltpu.make_async_remote_copy(
            sbuf.at[at], rbuf.at[at], send_more if e == WITH_ROWS else send, recv.at[e * 32 + off],
            device_id={"shard": peer}, device_id_type=MESH,
        )

    def send_piece(e, off):
        @pl.when(off != 0)
        def _():
            piece(e, off, ahead(me, off)).start()

    def code(x, inverse):
        share = jnp.maximum(jnp.abs(x) * inverse, 1e-30)
        level = jnp.exp2(share * lax.rsqrt(share) * SPAN - HALF)
        return jnp.where(x < 0, -level, level).astype(BF16)

    def encode_first(e, off):
        j = ahead(me, off)
        tile = jnp.zeros((8, 128), F32) if e == 0 else ssum[off]
        for t in range(tiles):
            x = latest(e, j, t)
            total = jnp.sum(x * x, axis=1, keepdims=True)
            tile = jnp.where(lanes == e * tiles + t, total, tile)
            sbuf[e * 32 + off, t] = code(x, lax.rsqrt(jnp.maximum(total, TINY)))
        ssum[off] = tile

    def encode(e, off):
        j = ahead(me, off)
        inverse = lax.rsqrt(jnp.maximum(ssum[off], TINY))
        for t in range(tiles):
            sbuf[e * 32 + off, t] = code(latest(e, j, t), to_all_lanes(inverse, e * tiles + t))
        if e == WITH_ROWS:
            sbuf[e * 32 + off, tiles] = own_rows[...]

    def encode_all(e):
        def body(k, _):
            for step in range(2):
                (encode if e >= ALONE else encode_first)(e, turn(2 * k + step, e))

            @pl.when(k > 0)
            def _():
                for step in range(2):
                    send_piece(e, turn(2 * k - 2 + step, e))

            return 0

        lax.fori_loop(0, 16, body, 0)
        for i in (30, 31):
            send_piece(e, turn(i, e))

    small = [
        pltpu.make_async_copy(weight_in, weight, small_sem.at[0]),
        pltpu.make_async_copy(gain_in, gain, small_sem.at[1]),
    ]
    for copy in small:
        copy.start()

    to_pair = pltpu.make_async_remote_copy(
        part, pair, pair_send, pair_recv, device_id={"expert": across}, device_id_type=MESH
    )
    w = 0
    for k, stage in enumerate(STAGES):
        for first, word in zip([True] + [False] * len(stage), stage):
            wait_first(w)
            w += 1
            for off in word:
                encode_first(0, off)
            if first:
                if k == 0:
                    pl.semaphore_wait(barrier, len(NEAR) + 2)
                else:
                    pl.semaphore_wait(stage_sem.at[k - 1], len(NEAR))
                if k < len(STAGES) - 1:
                    for off in NEAR:
                        pl.semaphore_signal(
                            stage_sem.at[k], inc=1, device_id={"shard": ahead(me, off)}, device_id_type=MESH
                        )
            for off in word:
                if off:
                    send_piece(0, off)
        if k == 0:
            for copy in small:
                copy.wait()
            own = weight[...] * gain[...]
            part[...] = jnp.concatenate([own, jnp.zeros_like(own)], axis=0).astype(BF16)
            for of_expert in loads:
                for copy in of_expert:
                    copy.start()

    to_pair.start()
    for copy in loads[0]:
        copy.wait()
    encode_all(1)
    for e in range(ALONE, experts):
        sums_of(e)

    to_pair.wait()
    mine, theirs = part[...].astype(F32)[:4], pair[...].astype(F32)[:4]
    low = jnp.where(y_lo == 0, mine, theirs)
    high = jnp.where(y_lo == 0, theirs, mine)
    own_rows[...] = jnp.concatenate([low, high], axis=0).astype(BF16)

    rsum[0] = ssum[0]

    def send_sums(i, _):
        off = turn(i, 0)

        @pl.when(off != 0)
        def _():
            pltpu.make_async_remote_copy(
                ssum.at[off], rsum.at[off], sum_send, sum_recv,
                device_id={"shard": ahead(me, off)}, device_id_type=MESH,
            ).start()

        return 0

    lax.fori_loop(0, 32, send_sums, 0)
    for e in range(ALONE, experts):
        encode_all(e)
    keep = []
    for e in range(experts):
        at = (e * 32, tiles_of(e))
        keep.append(pltpu.make_async_copy(sbuf.at[at], rbuf.at[at], self_sem.at[e]))
        keep[e].start()

    def arrival(e, off):
        @pl.when(off != 0)
        def _():
            piece(e, off, behind(me, off)).wait_recv()

    all_sums = pltpu.make_async_remote_copy(
        ssum.at[pl.ds(1, 31)], rsum.at[pl.ds(1, 31)], sum_send, sum_recv,
        device_id={"shard": ahead(me, 1)}, device_id_type=MESH,
    )
    all_sums.wait_recv()
    total = lax.fori_loop(1, 32, lambda k, acc: acc + rsum[k], rsum[0])

    def factors(k, _):
        fbuf[k] = jnp.sqrt(rsum[k] / total)
        return 0

    lax.fori_loop(0, 32, factors, 0)
    norm = jnp.sqrt(total)
    wide = lax.broadcasted_iota(jnp.int32, (8, 256), 1) - lax.broadcasted_iota(jnp.int32, (8, 256), 0)
    for e in range(experts):
        spread = jnp.zeros((8, 256), F32)
        for t in range(tiles):
            column = norm[:, e * tiles + t : e * tiles + t + 1]
            spread = jnp.where(wide == t * 8, column, spread)
        scale[e : e + 1, :] = jnp.sum(spread, axis=0, keepdims=True)[:, : tiles * 8]

    def decode(e, after_first=None):
        def body(k, _):
            offs = [turn(2 * k + step, e) for step in range(2)]
            for off in offs:
                arrival(e, off)
            for off in offs:
                factor = fbuf[off]
                source = behind(me, off)
                for t in range(tiles):
                    y = rbuf[e * 32 + off, t].astype(F32)
                    root = jnp.log(jnp.abs(y)) * (1.0 / (SPAN * LN2)) + HALF / SPAN
                    value = root * root * to_all_lanes(factor, e * tiles + t)
                    ready[e, t, source] = jnp.where(y < 0, -value, value).astype(BF16)
            return 0

        keep[e].wait()
        if after_first is None:
            lax.fori_loop(0, 16, body, 0)
        else:
            body(0, 0)
            after_first()
            lax.fori_loop(1, 16, body, 0)

    for e in range(WITH_ROWS + 1):
        decode(e)

    def take_rows(k, _):
        rows_in[k] = rbuf[WITH_ROWS * 32 + k, tiles]
        return 0

    lax.fori_loop(0, 32, take_rows, 0)
    to_core = pltpu.make_async_remote_copy(
        rows_in, rows_out, core_send, core_recv, device_id={"expert": beside}, device_id_type=MESH
    )
    for e in range(WITH_ROWS + 1, experts):
        decode(e, to_core.start)
    to_core.wait()

    def place(k, _):
        a, b = rows_in[k].astype(F32), rows_out[k].astype(F32)
        first = jnp.where(core == 0, a, b)
        second = jnp.where(core == 0, b, a)
        block = jnp.concatenate([first[:4], second[:4], first[4:], second[4:]], axis=0)
        router[:, pl.ds(pl.multiple_of(behind(me, k) * 128, 128), 128)] = block.astype(BF16)
        return 0

    lax.fori_loop(0, 32, place, 0)
    all_sums.wait_send()

    others = [e for e in range(experts) if e != WITH_ROWS]
    at = (pl.ds(0, 31 * len(others)), pl.ds(0, tiles))
    pltpu.make_async_remote_copy(
        sbuf.at[at], rbuf.at[at], send, recv.at[0], device_id={"shard": ahead(me, 1)}, device_id_type=MESH
    ).wait_send()
    at = (pl.ds(0, 31), tiles_of(WITH_ROWS))
    pltpu.make_async_remote_copy(
        sbuf.at[at], rbuf.at[at], send_more, recv.at[0], device_id={"shard": ahead(me, 1)}, device_id_type=MESH
    ).wait_send()


def deliver(ready_in, scale_in, router_in, ready, scale, router, sems):
    experts, tiles = ready.shape[:2]
    copies = [
        pltpu.make_async_copy(scale_in, scale, sems.at[experts * CHUNKS]),
        pltpu.make_async_copy(router_in, router, sems.at[experts * CHUNKS + 1]),
    ]
    for k in range(experts * CHUNKS):
        at = (k // CHUNKS, pl.ds(k % CHUNKS * (tiles // CHUNKS), tiles // CHUNKS))
        copies.append(pltpu.make_async_copy(ready_in.at[at], ready.at[at], sems.at[k]))
    for copy in copies:
        copy.start()
    for copy in copies:
        copy.wait()


def per_device(train_down, other_down, router_weight, router_gain):
    experts, inner, columns = train_down.shape
    tiles = inner // 32 // 8
    rows = inner // 8
    train = train_down.reshape(experts, rows, 8, columns)
    other = other_down.reshape(experts, rows, 8, columns)
    vmem = pl.BlockSpec(memory_space=pltpu.VMEM)
    anywhere = pl.BlockSpec(memory_space=pl.ANY)
    dma = pltpu.SemaphoreType.DMA
    pieces = experts * 32
    inside = pl.pallas_call(
        exchange,
        out_shape=(
            pltpu.VMEM((experts, tiles, 32, 8, columns), BF16),
            pltpu.VMEM((experts, tiles * 8), F32),
            pltpu.VMEM((16, 4096), BF16),
        ),
        in_specs=[anywhere, anywhere, anywhere, anywhere],
        out_specs=(vmem, vmem, vmem),
        scratch_shapes=[
            pltpu.VMEM((experts, columns), F32),
            pltpu.VMEM((1, columns), F32),
            dma((2,)),
            pltpu.VMEM((experts, rows, 8, columns), F32),
            pltpu.VMEM((experts, rows, 8, columns), BF16),
            pltpu.VMEM((pieces, tiles + EXTRA, 8, columns), BF16),
            pltpu.VMEM((pieces, tiles + EXTRA, 8, columns), BF16),
            pltpu.VMEM((32, 8, 128), F32),
            pltpu.VMEM((32, 8, 128), F32),
            pltpu.VMEM((32, 8, 128), F32),
            pltpu.VMEM((8, 128), BF16),
            pltpu.VMEM((8, 128), BF16),
            pltpu.VMEM((8, 128), BF16),
            pltpu.VMEM((32, 8, 128), BF16),
            pltpu.VMEM((32, 8, 128), BF16),
            dma((sum(map(len, STAGES)),)), dma((sum(map(len, STAGES)),)),
            dma(((experts - 1) * CHUNKS,)), dma(((experts - 1) * CHUNKS,)),
            pltpu.SemaphoreType.REGULAR((len(STAGES) - 1,)), dma, dma, dma((pieces,)), dma((experts,)),
            dma, dma, dma, dma, dma, dma,
        ],
        compiler_params=pltpu.CompilerParams(
            collective_id=0, has_side_effects=True, vmem_limit_bytes=48 * 1024 * 1024
        ),
        name="exchange",
    )(train, other, router_weight.T, router_gain.reshape(1, -1))
    ready, scale, router = pl.pallas_call(
        deliver,
        out_shape=(
            jax.ShapeDtypeStruct((experts, tiles, 32, 8, columns), BF16),
            jax.ShapeDtypeStruct((experts, tiles * 8), F32),
            jax.ShapeDtypeStruct((16, 4096), BF16),
        ),
        in_specs=[vmem, vmem, vmem],
        out_specs=(anywhere, anywhere, anywhere),
        scratch_shapes=[dma((experts * CHUNKS + 2,))],
        compiler_params=pltpu.CompilerParams(vmem_limit_bytes=16 * 1024 * 1024),
        name="deliver",
    )(*inside)
    ready = ready.transpose(0, 1, 3, 2, 4).reshape(experts, tiles * 8, 32 * columns)
    return (ready, scale, router.T)


def solution(mesh):
    in_specs = (
        P("expert", None, "shard"),
        P("expert", None, "shard"),
        P("shard", "expert"),
        P("shard"),
    )
    out_specs = (P("expert", "shard", None), P("expert", "shard"), P())
    return jax.shard_map(
        per_device, mesh=mesh, in_specs=in_specs, out_specs=out_specs, check_vma=False
    )
```

```python
import functools

import jax
import jax.numpy as jnp
from jax import lax
from jax.experimental import pallas as pl
from jax.experimental.pallas import tpu as pltpu
from jax.sharding import PartitionSpec as P

MESH = pl.DeviceIdType.MESH
F32 = jnp.float32
BF16 = jnp.bfloat16
SPAN = 240.0
HALF = 120.0
LN2 = 0.6931471805599453
TINY = 1e-37
CHUNKS = 5
ALONE = 2
WITH_ROWS = 2
EXTRA = 1
STRIDE = (27, 27, 27, 27)
SHIFT = (0, 10, 7, 20)


def coords(shard):
    return shard // 8, (shard // 4) % 2, shard % 4


def ahead(me, off):
    z, y, x = coords(me)
    dz, dy, dx = coords(off)
    return ((z + dz) % 4) * 8 + ((y + dy) % 2) * 4 + (x + dx) % 4


def behind(me, off):
    z, y, x = coords(me)
    dz, dy, dx = coords(off)
    return ((z + 4 - dz) % 4) * 8 + ((y + 2 - dy) % 2) * 4 + (x + 4 - dx) % 4


def steps_to(off):
    dz, dy, dx = coords(off)
    return min(dz, 4 - dz) + dy + min(dx, 4 - dx)


def in_words(k):
    offs = sorted(off for off in range(32) if steps_to(off) == k)
    offs = sorted(offs, key=lambda off: off * 11 % 32)
    return [offs[i : i + 5] for i in range(0, len(offs), 5)]


STAGES = [in_words(k) for k in range(1, 6)]
STAGES[-1][-1].append(0)
NEAR = STAGES[0][0]


def each(word, body):
    def step(_, rest):
        body(rest % 32)
        return rest // 32

    lax.fori_loop(0, len(word), step, jnp.int32(sum(off * 32**i for i, off in enumerate(word))))


def turn(i, e):
    return (STRIDE[e] * (i + 1) + SHIFT[e]) % 32


def to_all_lanes(tile, lane):
    return jnp.broadcast_to(tile[:, lane : lane + 1], tile.shape)


def exchange(train, other, weight_in, gain_in, ready, scale, router,
             weight, gain, small_sem, tbuf, obuf, sbuf, rbuf, ssum, rsum, fbuf, part, pair, own_rows, rows_in, rows_out,
             first_t, first_o, load_t, load_o, stage_sem, send, send_more, recv, self_sem,
             sum_send, sum_recv, pair_send, pair_recv, core_send, core_recv):
    experts, tiles = ready.shape[0], ready.shape[1]
    me = lax.axis_index("shard")
    group = lax.axis_index("expert")
    y_lo, core = group // 2, group % 2
    across = (1 - y_lo) * 2 + core
    beside = y_lo * 2 + (1 - core)

    barrier = pltpu.get_barrier_semaphore()
    for off in NEAR:
        pl.semaphore_signal(barrier, inc=1, device_id={"shard": ahead(me, off)}, device_id_type=MESH)
    for peer in (across, beside):
        pl.semaphore_signal(barrier, inc=1, device_id={"expert": peer}, device_id_type=MESH)

    words = [word for stage in STAGES for word in stage]
    for w, word in enumerate(words):
        def load_piece(off):
            at = pl.ds(ahead(me, off) * tiles, tiles)
            pltpu.make_async_copy(train.at[0, at], tbuf.at[0, at], first_t.at[w]).start()
            pltpu.make_async_copy(other.at[0, at], obuf.at[0, at], first_o.at[w]).start()

        each(word, load_piece)

    def wait_first(w):
        at = pl.ds(0, len(words[w]) * tiles)
        pltpu.make_async_copy(train.at[0, at], tbuf.at[0, at], first_t.at[w]).wait()
        pltpu.make_async_copy(other.at[0, at], obuf.at[0, at], first_o.at[w]).wait()

    loads = []
    for e in range(1, experts):
        of_expert = []
        for c in range(CHUNKS):
            part_of = pl.ds(c * (tiles * 32 // CHUNKS), tiles * 32 // CHUNKS)
            k = (e - 1) * CHUNKS + c
            of_expert += [
                pltpu.make_async_copy(train.at[e, part_of], tbuf.at[e, part_of], load_t.at[k]),
                pltpu.make_async_copy(other.at[e, part_of], obuf.at[e, part_of], load_o.at[k]),
            ]
        loads.append(of_expert)

    lanes = lax.broadcasted_iota(jnp.int32, (8, 128), 1)

    def latest(e, j, t):
        at = j * tiles + t
        return tbuf[e, at] + obuf[e, at].astype(F32)

    def sums_of(e):
        def body(k, _):
            for off in [k * 4 + step for step in range(4)]:
                j = ahead(me, off)
                tile = ssum[off]
                for t in range(tiles):
                    x = latest(e, j, t)
                    total = jnp.sum(x * x, axis=1, keepdims=True)
                    tile = jnp.where(lanes == e * tiles + t, total, tile)
                ssum[off] = tile
            return 0

        for copy in loads[e - 1]:
            copy.wait()
        lax.fori_loop(0, 8, body, 0)

    def tiles_of(e):
        return pl.ds(0, tiles + EXTRA if e == WITH_ROWS else tiles)

    def piece(e, off, peer):
        at = (e * 32 + off, tiles_of(e))
        return pltpu.make_async_remote_copy(
            sbuf.at[at], rbuf.at[at], send_more if e == WITH_ROWS else send, recv.at[e * 32 + off],
            device_id={"shard": peer}, device_id_type=MESH,
        )

    def send_piece(e, off):
        @pl.when(off != 0)
        def _():
            piece(e, off, ahead(me, off)).start()

    def code(x, inverse):
        share = jnp.maximum(jnp.abs(x) * inverse, 1e-30)
        level = jnp.exp2(share * lax.rsqrt(share) * SPAN - HALF)
        return jnp.where(x < 0, -level, level).astype(BF16)

    def encode_first(e, off):
        j = ahead(me, off)
        tile = jnp.zeros((8, 128), F32) if e == 0 else ssum[off]
        for t in range(tiles):
            x = latest(e, j, t)
            total = jnp.sum(x * x, axis=1, keepdims=True)
            tile = jnp.where(lanes == e * tiles + t, total, tile)
            sbuf[e * 32 + off, t] = code(x, lax.rsqrt(jnp.maximum(total, TINY)))
        ssum[off] = tile

    def encode(e, off):
        j = ahead(me, off)
        inverse = lax.rsqrt(jnp.maximum(ssum[off], TINY))
        for t in range(tiles):
            sbuf[e * 32 + off, t] = code(latest(e, j, t), to_all_lanes(inverse, e * tiles + t))
        if e == WITH_ROWS:
            sbuf[e * 32 + off, tiles] = own_rows[...]

    def encode_all(e):
        def body(k, _):
            for step in range(2):
                (encode if e >= ALONE else encode_first)(e, turn(2 * k + step, e))

            @pl.when(k > 0)
            def _():
                for step in range(2):
                    send_piece(e, turn(2 * k - 2 + step, e))

            return 0

        lax.fori_loop(0, 16, body, 0)
        for i in (30, 31):
            send_piece(e, turn(i, e))

    small = [
        pltpu.make_async_copy(weight_in, weight, small_sem.at[0]),
        pltpu.make_async_copy(gain_in, gain, small_sem.at[1]),
    ]
    for copy in small:
        copy.start()

    to_pair = pltpu.make_async_remote_copy(
        part, pair, pair_send, pair_recv, device_id={"expert": across}, device_id_type=MESH
    )
    w = 0
    for k, stage in enumerate(STAGES):
        for first, word in zip([True] + [False] * len(stage), stage):
            wait_first(w)
            w += 1
            for off in word:
                encode_first(0, off)
            if first:
                if k == 0:
                    pl.semaphore_wait(barrier, len(NEAR) + 2)
                else:
                    pl.semaphore_wait(stage_sem.at[k - 1], len(NEAR))
                if k < len(STAGES) - 1:
                    for off in NEAR:
                        pl.semaphore_signal(
                            stage_sem.at[k], inc=1, device_id={"shard": ahead(me, off)}, device_id_type=MESH
                        )
            for off in word:
                if off:
                    send_piece(0, off)
        if k == 0:
            for copy in small:
                copy.wait()
            own = weight[...] * gain[...]
            part[...] = jnp.concatenate([own, jnp.zeros_like(own)], axis=0).astype(BF16)
            for of_expert in loads:
                for copy in of_expert:
                    copy.start()

    to_pair.start()
    for copy in loads[0]:
        copy.wait()
    encode_all(1)
    for e in range(ALONE, experts):
        sums_of(e)

    to_pair.wait()
    mine, theirs = part[...].astype(F32)[:4], pair[...].astype(F32)[:4]
    low = jnp.where(y_lo == 0, mine, theirs)
    high = jnp.where(y_lo == 0, theirs, mine)
    own_rows[...] = jnp.concatenate([low, high], axis=0).astype(BF16)

    rsum[0] = ssum[0]

    def send_sums(i, _):
        off = turn(i, 0)

        @pl.when(off != 0)
        def _():
            pltpu.make_async_remote_copy(
                ssum.at[off], rsum.at[off], sum_send, sum_recv,
                device_id={"shard": ahead(me, off)}, device_id_type=MESH,
            ).start()

        return 0

    lax.fori_loop(0, 32, send_sums, 0)
    for e in range(ALONE, experts):
        encode_all(e)
    keep = []
    for e in range(experts):
        at = (e * 32, tiles_of(e))
        keep.append(pltpu.make_async_copy(sbuf.at[at], rbuf.at[at], self_sem.at[e]))
        keep[e].start()

    def arrival(e, off):
        @pl.when(off != 0)
        def _():
            piece(e, off, behind(me, off)).wait_recv()

    all_sums = pltpu.make_async_remote_copy(
        ssum.at[pl.ds(1, 31)], rsum.at[pl.ds(1, 31)], sum_send, sum_recv,
        device_id={"shard": ahead(me, 1)}, device_id_type=MESH,
    )
    all_sums.wait_recv()
    total = lax.fori_loop(1, 32, lambda k, acc: acc + rsum[k], rsum[0])

    def factors(k, _):
        fbuf[k] = jnp.sqrt(rsum[k] / total)
        return 0

    lax.fori_loop(0, 32, factors, 0)
    norm = jnp.sqrt(total)
    wide = lax.broadcasted_iota(jnp.int32, (8, 256), 1) - lax.broadcasted_iota(jnp.int32, (8, 256), 0)
    for e in range(experts):
        spread = jnp.zeros((8, 256), F32)
        for t in range(tiles):
            column = norm[:, e * tiles + t : e * tiles + t + 1]
            spread = jnp.where(wide == t * 8, column, spread)
        scale[e : e + 1, :] = jnp.sum(spread, axis=0, keepdims=True)[:, : tiles * 8]

    def decode(e, after_first=None):
        def body(k, _):
            offs = [turn(2 * k + step, e) for step in range(2)]
            for off in offs:
                arrival(e, off)
            for off in offs:
                factor = fbuf[off]
                source = behind(me, off)
                for t in range(tiles):
                    y = rbuf[e * 32 + off, t].astype(F32)
                    root = jnp.log(jnp.abs(y)) * (1.0 / (SPAN * LN2)) + HALF / SPAN
                    value = root * root * to_all_lanes(factor, e * tiles + t)
                    ready[e, t, source] = jnp.where(y < 0, -value, value).astype(BF16)
            return 0

        keep[e].wait()
        if after_first is None:
            lax.fori_loop(0, 16, body, 0)
        else:
            body(0, 0)
            after_first()
            lax.fori_loop(1, 16, body, 0)

    for e in range(WITH_ROWS + 1):
        decode(e)

    def take_rows(k, _):
        rows_in[k] = rbuf[WITH_ROWS * 32 + k, tiles]
        return 0

    lax.fori_loop(0, 32, take_rows, 0)
    to_core = pltpu.make_async_remote_copy(
        rows_in, rows_out, core_send, core_recv, device_id={"expert": beside}, device_id_type=MESH
    )
    for e in range(WITH_ROWS + 1, experts):
        decode(e, to_core.start)
    to_core.wait()

    def place(k, _):
        a, b = rows_in[k].astype(F32), rows_out[k].astype(F32)
        first = jnp.where(core == 0, a, b)
        second = jnp.where(core == 0, b, a)
        block = jnp.concatenate([first[:4], second[:4], first[4:], second[4:]], axis=0)
        router[:, pl.ds(pl.multiple_of(behind(me, k) * 128, 128), 128)] = block.astype(BF16)
        return 0

    lax.fori_loop(0, 32, place, 0)
    all_sums.wait_send()

    others = [e for e in range(experts) if e != WITH_ROWS]
    at = (pl.ds(0, 31 * len(others)), pl.ds(0, tiles))
    pltpu.make_async_remote_copy(
        sbuf.at[at], rbuf.at[at], send, recv.at[0], device_id={"shard": ahead(me, 1)}, device_id_type=MESH
    ).wait_send()
    at = (pl.ds(0, 31), tiles_of(WITH_ROWS))
    pltpu.make_async_remote_copy(
        sbuf.at[at], rbuf.at[at], send_more, recv.at[0], device_id={"shard": ahead(me, 1)}, device_id_type=MESH
    ).wait_send()


def deliver(ready_in, scale_in, router_in, ready, scale, router, sems):
    experts = ready.shape[0]
    copies = [pltpu.make_async_copy(ready_in.at[e], ready.at[e], sems.at[e]) for e in range(experts)]
    copies += [
        pltpu.make_async_copy(scale_in, scale, sems.at[experts]),
        pltpu.make_async_copy(router_in, router, sems.at[experts + 1]),
    ]
    for copy in copies:
        copy.start()
    for copy in copies:
        copy.wait()


def per_device(train_down, other_down, router_weight, router_gain):
    experts, inner, columns = train_down.shape
    tiles = inner // 32 // 8
    rows = inner // 8
    train = train_down.reshape(experts, rows, 8, columns)
    other = other_down.reshape(experts, rows, 8, columns)
    vmem = pl.BlockSpec(memory_space=pltpu.VMEM)
    anywhere = pl.BlockSpec(memory_space=pl.ANY)
    dma = pltpu.SemaphoreType.DMA
    pieces = experts * 32
    inside = pl.pallas_call(
        exchange,
        out_shape=(
            pltpu.VMEM((experts, tiles, 32, 8, columns), BF16),
            pltpu.VMEM((experts, tiles * 8), F32),
            pltpu.VMEM((16, 4096), BF16),
        ),
        in_specs=[anywhere, anywhere, anywhere, anywhere],
        out_specs=(vmem, vmem, vmem),
        scratch_shapes=[
            pltpu.VMEM((experts, columns), F32),
            pltpu.VMEM((1, columns), F32),
            dma((2,)),
            pltpu.VMEM((experts, rows, 8, columns), F32),
            pltpu.VMEM((experts, rows, 8, columns), BF16),
            pltpu.VMEM((pieces, tiles + EXTRA, 8, columns), BF16),
            pltpu.VMEM((pieces, tiles + EXTRA, 8, columns), BF16),
            pltpu.VMEM((32, 8, 128), F32),
            pltpu.VMEM((32, 8, 128), F32),
            pltpu.VMEM((32, 8, 128), F32),
            pltpu.VMEM((8, 128), BF16),
            pltpu.VMEM((8, 128), BF16),
            pltpu.VMEM((8, 128), BF16),
            pltpu.VMEM((32, 8, 128), BF16),
            pltpu.VMEM((32, 8, 128), BF16),
            dma((sum(map(len, STAGES)),)), dma((sum(map(len, STAGES)),)),
            dma(((experts - 1) * CHUNKS,)), dma(((experts - 1) * CHUNKS,)),
            pltpu.SemaphoreType.REGULAR((len(STAGES) - 1,)), dma, dma, dma((pieces,)), dma((experts,)),
            dma, dma, dma, dma, dma, dma,
        ],
        compiler_params=pltpu.CompilerParams(
            collective_id=0, has_side_effects=True, vmem_limit_bytes=48 * 1024 * 1024
        ),
        name="exchange",
    )(train, other, router_weight.T, router_gain.reshape(1, -1))
    ready, scale, router = pl.pallas_call(
        deliver,
        out_shape=(
            jax.ShapeDtypeStruct((experts, tiles, 32, 8, columns), BF16),
            jax.ShapeDtypeStruct((experts, tiles * 8), F32),
            jax.ShapeDtypeStruct((16, 4096), BF16),
        ),
        in_specs=[vmem, vmem, vmem],
        out_specs=(anywhere, anywhere, anywhere),
        scratch_shapes=[dma((experts + 2,))],
        compiler_params=pltpu.CompilerParams(vmem_limit_bytes=16 * 1024 * 1024),
        name="deliver",
    )(*inside)
    ready = ready.transpose(0, 1, 3, 2, 4).reshape(experts, tiles * 8, 32 * columns)
    return (ready, scale, router.T)


def solution(mesh):
    in_specs = (
        P("expert", None, "shard"),
        P("expert", None, "shard"),
        P("shard", "expert"),
        P("shard"),
    )
    out_specs = (P("expert", "shard", None), P("expert", "shard"), P())
    return jax.shard_map(
        per_device, mesh=mesh, in_specs=in_specs, out_specs=out_specs, check_vma=False
    )
```
